32 devices in a mesh: rep: 2 (over z, core), dp: 16 (over x, y).
Axes of the slice: x: 4, y: 4, z: 1, core: 2. Of those that a mesh axis runs over, the one named last changes fastest.
The devices are a block of a 4x4x8 slice.
Arguments:
- x: bfloat16 [32, 2048, 512], P(('rep', 'dp')), parts along dimension 0
- dy: bfloat16 [32, 2048, 512], P(('rep', 'dp')), parts along dimension 0
- w_gate: bfloat16 [2, 512, 1664], replicated
- w_up: bfloat16 [2, 512, 1664], replicated
- w_down: bfloat16 [2, 1664, 512], replicated
- m_w_gate: float32 [2, 512, 1664], replicated
- m_w_up: float32 [2, 512, 1664], replicated
- m_w_down: float32 [2, 1664, 512], replicated
- v_w_gate: float32 [2, 512, 1664], replicated
- v_w_up: float32 [2, 512, 1664], replicated
- v_w_down: float32 [2, 1664, 512], replicated
Outputs:
- output 1: bfloat16 [4, 512, 1664], P('rep'), parts along dimension 0
- output 2: bfloat16 [4, 512, 1664], P('rep'), parts along dimension 0
- output 3: bfloat16 [4, 1664, 512], P('rep'), parts along dimension 0
- output 4: float32 [4, 512, 1664], P('rep'), parts along dimension 0
- output 5: float32 [4, 512, 1664], P('rep'), parts along dimension 0
- output 6: float32 [4, 1664, 512], P('rep'), parts along dimension 0
- output 7: float32 [4, 512, 1664], P('rep'), parts along dimension 0
- output 8: float32 [4, 512, 1664], P('rep'), parts along dimension 0
- output 9: float32 [4, 1664, 512], P('rep'), parts along dimension 0
There are 2 independent parts. The reference program is written for one: setup_inputs(seed, part) draws one part's arguments, and reference() takes and returns one part's arrays. A program takes and returns all parts, laid end to end along the dimension named above; an argument that names none is the same for every part.
All inputs are finite; a program needn't handle non-finite values.
Results may differ from the reference program's by a relative error of at most 0.022.
Values are sent between devices in bfloat16 or wider.
A program may use at most 768 MiB of HBM per device.

```python
import jax
import jax.numpy as jnp
from jax import lax

SEQUENCES = 16
TOKENS = 2048
D = 512
FF = 1664
LAYERS = 2
NAMES = ("w_gate", "w_up", "w_down")
SHAPES = {"w_gate": (LAYERS, D, FF), "w_up": (LAYERS, D, FF), "w_down": (LAYERS, FF, D)}


def bump(key, n, height):
    away = (jnp.arange(n, dtype=jnp.int32) - jax.random.randint(key, (), 0, n, jnp.int32)) % n
    return jnp.where(away < n // 8, height, 1.0)


def together(key, own, strength):
    shared = jax.random.normal(key, own.shape[1:], jnp.float32)
    return (own + strength * shared) * lax.rsqrt(1 + strength * strength)


def setup_inputs(seed: int = 0, part: int = 0) -> dict:
    kx, kdy, ka, kb, kz, kf, kh, kl, *keys = jax.random.split(jax.random.key(seed), 8 + 3 * len(NAMES))
    kx, kdy, ka, kb = (jax.random.fold_in(k, part) for k in (kx, kdy, ka, kb))
    kw, km, kv = (keys[i::3] for i in range(3))
    shape = (SEQUENCES, TOKENS, D)
    much_x, much_dy = jax.random.uniform(kz, (2,), jnp.float32, 0.0, 1.0)
    loud = 2.0 ** jax.random.uniform(jax.random.fold_in(kz, 1), (), jnp.float32, -1.0, 2.0)
    layers = 2.0 ** jax.random.uniform(kl, (LAYERS, 1, 1), jnp.float32, -1.0, 1.0)
    x = together(ka, jax.random.normal(kx, shape, jnp.float32), much_x) * bump(kf, D, 4.0)
    dy = together(kb, jax.random.normal(kdy, shape, jnp.float32), much_dy)
    drawn = {"x": x.astype(jnp.bfloat16), "dy": (loud * dy * (SEQUENCES * TOKENS) ** -0.5).astype(jnp.bfloat16)}
    for key, name in zip(kw, NAMES, strict=True):
        w = jax.random.normal(key, SHAPES[name], jnp.float32) * SHAPES[name][1] ** -0.5
        drawn[name] = (w * {"w_gate": 1.0, "w_up": bump(kh, FF, 4.0), "w_down": layers}[name]).astype(jnp.bfloat16)
    for key, name in zip(km, NAMES, strict=True):
        drawn[f"m_{name}"] = 0.1 * jax.random.normal(key, SHAPES[name], jnp.float32)
    for key, name in zip(kv, NAMES, strict=True):
        drawn[f"v_{name}"] = jax.random.uniform(key, SHAPES[name], jnp.float32, 0.005, 0.015)
    return drawn


def matmul(a, w):
    return jnp.dot(a, w, preferred_element_type=jnp.float32).astype(jnp.bfloat16)


def normed(h):
    wide = h.astype(jnp.float32)
    scale = lax.rsqrt(jnp.mean(wide**2, -1, keepdims=True) + 1e-6)
    return (wide * scale).astype(jnp.bfloat16)


def layer(h, w):
    a = normed(h)
    gate = jnp.dot(a, w["w_gate"], preferred_element_type=jnp.float32)
    up = jnp.dot(a, w["w_up"], preferred_element_type=jnp.float32)
    return h + matmul((jax.nn.silu(gate) * up).astype(jnp.bfloat16), w["w_down"])


def adamw(w, m, v, g):
    m = 0.9 * m + 0.1 * g
    v = 0.95 * v + 0.05 * g * g
    step = m * lax.rsqrt(v + 1e-8) + 0.1 * w
    return (w - 0.02 * step).astype(jnp.bfloat16), m, v


def clipped(gradients, sum_of_squares, count):
    factor = jnp.minimum(1.0, 0.5 * lax.rsqrt(sum_of_squares / count + 1e-30))
    return [g * factor for g in gradients]


def stack(weights, h):
    return lax.scan(lambda h, w: (layer(h, w), None), h, weights)[0]


def reference(x, dy, w_gate, w_up, w_down, m_w_gate, m_w_up, m_w_down, v_w_gate, v_w_up, v_w_down):
    weights = dict(zip(NAMES, (w_gate, w_up, w_down), strict=True))

    def take(so_far, sequence):
        h, by_y = sequence
        _, back = jax.vjp(lambda w: stack(w, h), weights)
        return jax.tree.map(lambda total, term: total + term.astype(jnp.float32), so_far, back(by_y)[0]), None

    none_yet = {name: jnp.zeros(w.shape, jnp.float32) for name, w in weights.items()}
    by_weights, _ = lax.scan(take, none_yet, (x, dy))
    gradients = [by_weights[name].astype(jnp.bfloat16).astype(jnp.float32) for name in NAMES]
    gradients = clipped(gradients, sum(jnp.sum(g * g) for g in gradients), sum(g.size for g in gradients))
    new = [
        adamw(w.astype(jnp.float32), m, v, g)
        for w, m, v, g in zip((w_gate, w_up, w_down), (m_w_gate, m_w_up, m_w_down), (v_w_gate, v_w_up, v_w_down), gradients, strict=True)
    ]
    return tuple(one[which] for which in range(3) for one in new)
```

```python
import functools
import jax
import jax.numpy as jnp
from jax import lax
from jax.experimental import pallas as pl
from jax.experimental.pallas import tpu as pltpu
from jax.sharding import PartitionSpec as P

MESH = pl.DeviceIdType.MESH
LANES = 128
BLOCK = 1024
PARTS = ((1.5, 0.7, 0.7, 0.4), (2.1, 1.1, 1.2, 0.6))
F32, BF16 = jnp.float32, jnp.bfloat16


def block_rows(n, most=256):
    return max(b for b in range(8, most + 1, 8) if n % b == 0)


def halves(c):
    a = (c // 2 + 15) // 16 * 16
    return a, c - a


class Plan:
    SLOTS = 3

    def __init__(self, units, run, tiles, side):
        self.side = side
        self.units = []
        self.rows = len({layer for layer, _ in units}) * tiles * run
        r1 = r2 = sem = 0
        most = max(count for _, count in units) * run // 2 // side
        row = {layer: layer * tiles * run for layer, _ in units}
        for u, (layer, count) in enumerate(units):
            h = count * run // 2
            c1 = h // side
            c2 = c1 // side
            streams = []
            for s in range(2):
                acc = (2 * (u % self.SLOTS) + s) * most
                streams.append(dict(base=row[layer] + s * h, h=h, c1=c1, c2=c2, r1=r1, r2=r2, sem=sem, acc=acc, s=s))
                r1 += 3 * c1
                r2 += 3 * c2
                sem += 20
            self.units.append(streams)
            row[layer] += 2 * h
        self.r1, self.r2, self.acc, self.sems = r1, r2, 2 * self.SLOTS * most, sem


class Comm:
    def __init__(self, plan, lg, gathered, r1, r2, acc, squares, send, recv):
        self.plan, self.lg, self.g, self.r1, self.r2, self.acc = plan, lg, gathered, r1, r2, acc
        self.squares, self.send, self.recv = squares, send, recv
        side = plan.side
        me = lax.axis_index("dp")
        self.x, self.y = me // side, me % side
        self.live = []

    def at(self, ring, step):
        side = self.plan.side
        if ring == 0:
            return {"dp": lax.rem(self.x + (step + side), side) * side + self.y}
        return {"dp": self.x * side + lax.rem(self.y + (step + side), side)}

    def barrier(self):
        sem = pltpu.get_barrier_semaphore()
        for ring in range(2):
            for step in range(1, self.plan.side):
                pl.semaphore_signal(sem, inc=1, device_id=self.at(ring, step), device_id_type=MESH)
        pl.semaphore_wait(sem, 2 * (self.plan.side - 1))

    def copy(self, src, dst, k, device):
        return pltpu.make_async_remote_copy(
            src_ref=src, dst_ref=dst, send_sem=self.send.at[k], recv_sem=self.recv.at[k], device_id=device, device_id_type=MESH
        )

    def go(self, *args):
        c = self.copy(*args)
        c.start()
        self.live.append(c)
        return c

    def finish(self):
        for c in self.live:
            c.wait_send()

    def ring(self, st, phase):
        ring = st["s"] if phase == 0 else 1 - st["s"]
        return ring, (self.x if ring == 0 else self.y)

    def geometry(self, st, phase):
        side = self.plan.side
        if phase == 0:
            return st["base"], st["c1"], self.r1, st["r1"], st["sem"]
        _, p = self.ring(st, 0)
        return st["base"] + p * st["c1"], st["c2"], self.r2, st["r2"], st["sem"] + 6

    def rows(self, ref, start, n):
        return ref.at[pl.ds(pl.multiple_of(start, 8), n), :]

    def place(self, st, phase, step):
        base, c, *_ = self.geometry(st, phase)
        _, p = self.ring(st, phase)
        return base + lax.rem(p + (step + self.plan.side), self.plan.side) * c

    def rs_start(self, st, phase):
        base, c, r, r0, k = self.geometry(st, phase)
        ring, p = self.ring(st, phase)
        a, b = halves(c)
        right, left = self.at(ring, 1), self.at(ring, -1)
        far, near_r, near_l = self.place(st, phase, 2), self.place(st, phase, 1), self.place(st, phase, -1)
        out = {}
        out[0] = self.go(self.rows(self.lg, far, a), self.rows(r, r0, a), k, right)
        out[2] = self.go(self.rows(self.lg, far + a, b), self.rows(r, r0 + a, b), k + 2, left)
        out[1] = self.go(self.rows(self.lg, near_r + a, b), self.rows(r, r0 + c + a, b), k + 1, right)
        out[3] = self.go(self.rows(self.lg, near_l, a), self.rows(r, r0 + 2 * c, a), k + 3, left)
        st["out", phase] = out

    def add_loop(self, n, body):
        b = block_rows(n)

        def step(i, carry):
            body(i * b, b)
            return carry

        lax.fori_loop(0, n // b, step, 0)

    def load(self, ref, start, n):
        return ref[pl.ds(pl.multiple_of(start, 8), n), :]

    def rs_mid(self, st, phase):
        base, c, r, r0, k = self.geometry(st, phase)
        ring, p = self.ring(st, phase)
        a, b = halves(c)
        right, left = self.at(ring, 1), self.at(ring, -1)
        out = st["out", phase]
        for which, step, off, n, dst, device in ((0, 1, 0, a, r0 + c, right), (2, -1, a, b, r0 + 2 * c + a, left)):
            out[which].wait_recv()
            mine = self.place(st, phase, step) + off
            slot = r0 + off

            def body(o, m, mine=mine, slot=slot, off=off, step=step):
                if phase == 0:
                    own = self.load(self.lg, mine + o, m).astype(F32)
                else:
                    own = self.load(self.acc, st["acc"] + lax.rem(p + (step + self.plan.side), self.plan.side) * c + off + o, m)
                total = own + self.load(r, slot + o, m).astype(F32)
                self.lg[pl.ds(pl.multiple_of(mine + o, 8), m), :] = total.astype(BF16)

            self.add_loop(n, body)
            out[4 if which == 0 else 5] = self.go(self.rows(self.lg, mine, n), self.rows(r, dst, n), k + (4 if which == 0 else 5), device)

    def rs_end(self, st, phase):
        base, c, r, r0, k = self.geometry(st, phase)
        ring, p = self.ring(st, phase)
        out = st["out", phase]
        for which in (1, 3, 4, 5):
            out[which].wait_recv()
        mine = base + p * c

        def body(o, m):
            if phase == 0:
                own = self.load(self.lg, mine + o, m).astype(F32)
            else:
                own = self.load(self.acc, st["acc"] + p * c + o, m)
            total = own + self.load(r, r0 + c + o, m).astype(F32) + self.load(r, r0 + 2 * c + o, m).astype(F32)
            if phase == 0:
                self.acc[pl.ds(pl.multiple_of(st["acc"] + o, 8), m), :] = total
                self.lg[pl.ds(pl.multiple_of(mine + o, 8), m), :] = total.astype(BF16)
            else:
                rounded = total.astype(BF16)
                self.g[pl.ds(pl.multiple_of(mine + o, 8), m), :] = rounded
                wide = rounded.astype(F32)
                self.squares[...] += jnp.sum((wide * wide).reshape(m // 8, 8, LANES), axis=0)

        self.add_loop(c, body)

    def ag_geometry(self, st, level):
        phase = 1 - level
        base, c, *_ = self.geometry(st, phase)
        return phase, base, c, st["sem"] + 12 + 4 * level

    def ag_start(self, st, level):
        phase, base, c, k = self.ag_geometry(st, level)
        ring, p = self.ring(st, phase)
        here = self.rows(self.g, base + p * c, c)
        st["ag", level] = [self.go(here, here, k, self.at(ring, 1)), self.go(here, here, k + 1, self.at(ring, -1))]

    def ag_mid(self, st, level):
        phase, base, c, k = self.ag_geometry(st, level)
        ring, p = self.ring(st, phase)
        a, b = halves(c)
        st["ag", level][0].wait_recv()
        from_left = self.rows(self.g, self.place(st, phase, -1), a)
        first = self.go(from_left, from_left, k + 2, self.at(ring, 1))
        st["ag", level][1].wait_recv()
        from_right = self.rows(self.g, self.place(st, phase, 1) + a, b)
        second = self.go(from_right, from_right, k + 3, self.at(ring, -1))
        st["ag", level] = [first, second]

    def ag_end(self, st, level):
        for c in st["ag", level]:
            c.wait_recv()

    def norm_step(self, step, parts, send, recv):
        side = self.plan.side
        if step > 0:
            for c in self.copies:
                c.wait()
            total = parts[(step - 1) * side]
            for i in range(1, side):
                total = total + parts[(step - 1) * side + i]
            self.squares[...] = total
        if step < 2:
            slot = step * side + (self.x if step == 0 else self.y)
            parts[slot] = self.squares[...]
            self.copies = []
            for far in range(1, side):
                k = step * (side - 1) + far - 1
                here = parts.at[slot]
                c = pltpu.make_async_remote_copy(
                    src_ref=here, dst_ref=here, send_sem=send.at[k], recv_sem=recv.at[k], device_id=self.at(step, far), device_id_type=MESH
                )
                c.start()
                self.copies.append(c)

    def step(self, st, step):
        if step == 0:
            self.rs_start(st, 0)
        elif step in (1, 3):
            self.rs_mid(st, step // 2)
        elif step == 2:
            self.rs_end(st, 0)
            self.rs_start(st, 1)
        elif step == 4:
            self.rs_end(st, 1)
            self.ag_start(st, 0)
        elif step in (5, 7):
            self.ag_mid(st, step // 7)
        elif step == 6:
            self.ag_end(st, 0)
            self.ag_start(st, 1)
        else:
            self.ag_end(st, 1)


def update_kernel(count, squares, g, wg, wu, wd, mg, mu, md, vg, vu, vd, *outs):
    factor = jnp.minimum(1.0, 0.5 * lax.rsqrt(jnp.sum(squares[...]) / count + 1e-30))
    layers, d, _ = wg.shape
    blocks = wd.shape[2] // LANES

    def one(gradient, w, m, v):
        g = gradient.astype(F32) * factor
        new_m = 0.9 * m + 0.1 * g
        new_v = 0.95 * v + 0.05 * g * g
        step = new_m * lax.rsqrt(new_v + 1e-8) + 0.1 * w.astype(F32)
        return (w.astype(F32) - 0.02 * step).astype(BF16), new_m, new_v

    for layer in range(layers):
        for i, (w, m, v) in enumerate(((wg, mg, vg), (wu, mu, vu))):
            out = one(g[layer, pl.ds(i * d, d), :], w[layer], m[layer], v[layer])
            for o, value in zip((outs[i], outs[3 + i], outs[6 + i]), out, strict=True):
                o[layer] = value
        for c in range(blocks):
            cols = pl.ds(c * LANES, LANES)
            out = one(g[layer, pl.ds(2 * d + c * LANES, LANES), :], wd[layer, :, cols], md[layer, :, cols], vd[layer, :, cols])
            for o, value in zip((outs[2], outs[5], outs[8]), out, strict=True):
                o[layer, :, cols] = value


def update(gathered, squares, weights, m, v, count):
    layers, d, ff = weights[0].shape
    tiles = ff // LANES
    tile_rows = 3 * d
    wide = pl.BlockSpec((layers, d, LANES), lambda t: (0, 0, t))
    tall = pl.BlockSpec((layers, LANES, d), lambda t: (0, t, 0))
    three = [wide, wide, tall]
    return pl.pallas_call(
        functools.partial(update_kernel, count),
        name="update",
        grid=(tiles,),
        in_specs=[pl.BlockSpec((8, LANES), lambda t: (0, 0)), pl.BlockSpec((layers, tile_rows, LANES), lambda t: (0, t, 0)), *three * 3],
        out_specs=three * 3,
        out_shape=[jax.ShapeDtypeStruct(a.shape, a.dtype) for a in (*weights, *m, *v)],
        compiler_params=pltpu.CompilerParams(vmem_limit_bytes=60 * 2**20),
    )(squares, gathered.reshape(layers, tiles * tile_rows, LANES), *weights, *m, *v)


def dot(a, b):
    return jnp.dot(a, b, preferred_element_type=F32)


def dot_nt(a, b):
    return lax.dot_general(a, b, (((1,), (1,)), ((), ())), preferred_element_type=F32)


def row_loop(rows, block, body):
    def step(i, carry):
        body(pl.ds(pl.multiple_of(i * block, block), block))
        return carry

    lax.fori_loop(0, rows // block, step, 0)


def scale_of(wide):
    return lax.rsqrt(jnp.mean(wide * wide, -1, keepdims=True) + 1e-6)


def normalise(h, a, at):
    def body(rows):
        wide = h[rows, :].astype(F32)
        value = (wide * scale_of(wide)).astype(BF16)
        a[rows, :] = value
        at[:, rows] = value.T

    row_loop(h.shape[0], 256, body)


def transpose(src, dst):
    def body(rows):
        dst[:, rows] = src[rows, :].T

    row_loop(src.shape[0], 256, body)


def sigmoid(z):
    return 0.5 * jnp.tanh(0.5 * z) + 0.5


def column_tiles(ff):
    whole = ff // 256
    return [(i * 256, 256) for i in range(whole)] + ([(whole * 256, LANES)] if ff % 256 else [])


def forward(a, h, wg, wu, wd, out):
    def body(rows):
        block = a[rows, :]
        parts = []
        for start, width in column_tiles(wg.shape[1]):
            cols = pl.ds(start, width)
            gate, up = dot(block, wg[:, cols]), dot(block, wu[:, cols])
            parts.append((gate * sigmoid(gate) * up).astype(BF16))
        out[rows, :] = h[rows, :] + dot(jnp.concatenate(parts, axis=1), wd[...]).astype(BF16)

    row_loop(a.shape[0], 512, body)


def backward_tile(start, width, a, at, dy, dyt, wg, wu, wd, act, by_both, lg, row, by_input=None, pause=lambda part: None):
    cols = pl.ds(start, width)
    both = jnp.concatenate([wg[:, cols], wu[:, cols]], axis=1)
    down = wd[cols, :]

    def body(rows):
        hidden = dot(a[rows, :], both)
        gate, up = hidden[:, :width], hidden[:, width:]
        by_act = dot_nt(dy[rows, :], down).astype(BF16).astype(F32)
        s = sigmoid(gate)
        silu = gate * s
        act[rows, :width] = (silu * up).astype(BF16)
        by_gate = (by_act * up * (s + silu * (1.0 - s))).astype(BF16)
        by_up = (by_act * silu).astype(BF16)
        by_both[rows, :width] = by_gate
        by_both[rows, width : 2 * width] = by_up

    row_loop(a.shape[0], BLOCK, body)
    pause(0)
    if by_input:
        by_a, new = by_input

        def add(rows):
            term = dot_nt(by_both[rows, : 2 * width], both)
            by_a[rows, :] = term if new else by_a[rows, :] + term

        row_loop(a.shape[0], BLOCK, add)
        pause(1)
    d = wg.shape[0]
    out = dot(at[...], by_both[:, : 2 * width]).astype(BF16)
    for i in range(2):
        for j in range(width // LANES):
            lg[pl.ds(row + j * 3 * d + i * d, d), :] = out[:, i * width + j * LANES : i * width + (j + 1) * LANES]
    pause(2)
    out = dot(dyt[...], act[:, :width]).astype(BF16).T
    for j in range(width // LANES):
        for c in range(d // LANES):
            lg[pl.ds(row + j * 3 * d + 2 * d + c * LANES, LANES), :] = out[j * LANES : (j + 1) * LANES, c * LANES : (c + 1) * LANES]
    pause(3)


def backward_input(h, dy, by_a, dyt):
    d = h.shape[1]

    def body(rows):
        by = by_a[rows, :].astype(BF16).astype(F32)
        wide = h[rows, :].astype(F32)
        s = scale_of(wide)
        by_scale = jnp.sum(by * wide, -1, keepdims=True)
        by_wide = by * s - wide * (by_scale * s * s * s * (1.0 / d))
        value = dy[rows, :] + by_wide.astype(BF16)
        dy[rows, :] = value
        dyt[:, rows] = value.T

    row_loop(h.shape[0], 256, body)


class Schedule:
    RATE, LATENCY, COST, BACKLOG = 46600.0, 2.2, 0.3, 4.0

    def __init__(self, units):
        self.units = units
        self.now = self.free = 0.0
        self.due = {}
        self.squares = None
        self.out = []

    def send(self, rows):
        self.free = max(self.now, self.free) + rows * LANES * 2 / self.RATE
        return self.free + self.LATENCY

    def begin(self, u):
        self.run(u, 0)

    def run(self, u, step):
        st = self.units[u][0]
        c1, c2 = st["c1"], st["c2"]
        self.out.append((u, step))
        self.now += self.COST * (1 if step in (1, 2) else 0.3)
        sent = {0: (c1 // 2, c1 // 2), 1: (c1 // 2,), 2: (c2 // 2, c2 // 2), 3: (c2 // 2,), 4: (c2,), 5: (c2 // 2,), 6: (c1,), 7: (c1 // 2,)}
        times = [self.send(rows) for rows in sent.get(step, ())]
        if step < 8:
            self.due[u] = (step + 1, times[0])
        else:
            del self.due[u]

    def norm(self, step):
        self.out.append(("norm", step))
        self.now += 0.1
        if step < 2:
            self.squares = (step + 1, self.send(64) + 1.5)
        else:
            self.squares = ("done", 0.0)

    def choices(self):
        found = [
            (due, 0 if step <= 4 else 1 if step != 6 else 2, u, step)
            for u, (step, due) in self.due.items()
            if step != 2 or self.due.get(u - Plan.SLOTS, (5, 0))[0] > 4
        ]
        if self.squares and self.squares[0] != "done":
            found.append((self.squares[1], 0, "norm", self.squares[0]))
        return found

    def take(self, which, step):
        if which == "norm":
            self.norm(step)
        else:
            self.run(which, step)

    def compute(self, us):
        self.now += us
        while True:
            ready = [c for c in self.choices() if c[0] <= self.now and (c[3] != 6 or self.free - self.now < self.BACKLOG)]
            if not ready:
                return
            _, _, which, step = min(ready, key=lambda c: (c[1], c[0]))
            self.take(which, step)

    def drain(self):
        begun = False
        while self.due or not begun or self.squares[0] != "done":
            if not begun and all(step > 4 for step, _ in self.due.values()):
                begun = True
                self.norm(0)
                continue
            late = [c for c in self.choices() if c[3] != 6 or self.free - self.now < self.BACKLOG or len(self.due) == 1] or self.choices()
            due, _, which, step = min(late, key=lambda c: (max(c[0], self.now), c[1], c[0]))
            self.now = max(self.now, due)
            self.take(which, step)


def step_kernel(plan, counts, x_h, dy_h, wg_h, wu_h, wd_h, g_o, squares_out,
                h, dy, dyt, a, at, keep, wg, wu, wd, act, by_both, by_a,
                lg, gathered, r1, r2, acc, squares, parts, send, recv, nsend, nrecv, sem):
    comm = Comm(plan, lg, gathered, r1, r2, acc, squares, send, recv)
    layers, d, ff = wg.shape
    base = 3 * d * (ff // LANES)
    loads = [(x_h, h)] + [(w_h.at[0], w.at[0]) for w_h, w in ((wg_h, wg), (wu_h, wu), (wd_h, wd))]
    loads += [(w_h.at[1], w.at[1]) for w_h, w in ((wg_h, wg), (wu_h, wu), (wd_h, wd))]
    loads = [pltpu.make_async_copy(src, dst, sem.at[i]) for i, (src, dst) in enumerate(loads)]
    for c in loads:
        c.start()
    squares[...] = jnp.zeros_like(squares)
    comm.barrier()
    outs = []
    plan_at = Schedule(plan.units)
    plan_at.now = 20.0
    done = [0]

    def steps():
        for which, step in plan_at.out[done[0] :]:
            if which == "norm":
                comm.norm_step(step, parts, nsend, nrecv)
                continue
            unit = plan.units[which]
            for st in unit:
                comm.step(st, step)
            if step == 8:
                rows = pl.ds(unit[0]["base"], 2 * unit[0]["h"])
                c = pltpu.make_async_copy(gathered.at[rows, :], g_o.at[rows, :], sem.at[len(loads) + 2 + len(outs)])
                c.start()
                outs.append(c)
        done[0] = len(plan_at.out)

    def pause(width, part):
        plan_at.now += PARTS[width > LANES][part]
        if part < 3:
            plan_at.compute(0.0)
            steps()

    def tiles(layer, by_input):
        first = sum(len(c) for c in counts[layer + 1 :])
        end, u = counts[layer][0], 0
        for i, (start, width) in enumerate(column_tiles(ff)):
            backward_tile(
                start, width, a, at, dy, dyt, wg.at[layer], wu.at[layer], wd.at[layer], act, by_both, lg,
                layer * base + start // LANES * 3 * d, by_input and (by_a, i == 0), functools.partial(pause, width),
            )
            if (start + width) // LANES == end:
                plan_at.begin(first + u)
                u += 1
                end += counts[layer][u] if u < len(counts[layer]) else 0
            plan_at.compute(0.0)
            steps()

    loads[0].wait()
    normalise(h, a, at)
    for c in loads[1:4]:
        c.wait()
    forward(a, h, wg.at[0], wu.at[0], wd.at[0], keep)
    again = pltpu.make_async_copy(dy_h, dy, sem.at[len(loads)])
    again.start()
    normalise(keep, a, at)
    again.wait()
    transpose(dy, dyt)
    for c in loads[4:]:
        c.wait()
    tiles(1, True)
    again = pltpu.make_async_copy(x_h, h, sem.at[len(loads) + 1])
    again.start()
    backward_input(keep, dy, by_a, dyt)
    plan_at.compute(2.0)
    steps()
    again.wait()
    normalise(h, a, at)
    plan_at.compute(2.0)
    steps()
    tiles(0, False)
    plan_at.drain()
    steps()
    squares_out[...] = squares[...]
    for c in outs:
        c.wait()
    comm.finish()


def gradients(x, dy, wg, wu, wd, side):
    tokens, d = x.shape
    layers, _, ff = wg.shape
    tiles = ff // LANES
    counts = {layers - 1: [2, 4, 4, tiles - 10], 0: [4, 4, 4, tiles - 12]}
    plan = Plan([(layer, c) for layer in (layers - 1, 0) for c in counts[layer]], 3 * d, tiles, side)
    any_spec = pl.BlockSpec(memory_space=pl.ANY)
    flat, tall = pltpu.VMEM((tokens, d), BF16), pltpu.VMEM((d, tokens), BF16)
    tile = pltpu.VMEM((tokens, 256), BF16)
    return pl.pallas_call(
        functools.partial(step_kernel, plan, [counts[0], counts[layers - 1]]),
        name="gradients",
        out_shape=(jax.ShapeDtypeStruct((plan.rows, LANES), BF16), jax.ShapeDtypeStruct((8, LANES), F32)),
        in_specs=[any_spec] * 5,
        out_specs=(any_spec, pl.BlockSpec(memory_space=pltpu.VMEM)),
        scratch_shapes=[
            flat, flat, tall, flat, tall, flat,
            pltpu.VMEM(wg.shape, BF16),
            pltpu.VMEM(wu.shape, BF16),
            pltpu.VMEM(wd.shape, BF16),
            tile,
            pltpu.VMEM((tokens, 512), BF16),
            pltpu.VMEM((tokens, d), F32),
            pltpu.VMEM((plan.rows, LANES), BF16),
            pltpu.VMEM((plan.rows, LANES), BF16),
            pltpu.VMEM((plan.r1, LANES), BF16),
            pltpu.VMEM((plan.r2, LANES), BF16),
            pltpu.VMEM((plan.acc, LANES), F32),
            pltpu.VMEM((8, LANES), F32),
            pltpu.VMEM((2 * side, 8, LANES), F32),
            pltpu.SemaphoreType.DMA((plan.sems,)),
            pltpu.SemaphoreType.DMA((plan.sems,)),
            pltpu.SemaphoreType.DMA((2 * (side - 1),)),
            pltpu.SemaphoreType.DMA((2 * (side - 1),)),
            pltpu.SemaphoreType.DMA((9 + len(plan.units),)),
        ],
        compiler_params=pltpu.CompilerParams(collective_id=0, has_side_effects=True, vmem_limit_bytes=67043328),
    )(x, dy, wg, wu, wd)


def solution(mesh):
    n = mesh.shape["dp"]
    side = int(n**0.5)

    def step(x, dy, *arrays):
        weights, m, v = (arrays[i : i + 3] for i in (0, 3, 6))
        gathered, squares = gradients(x[0], dy[0], *weights, side)
        return tuple(update(gathered, squares, weights, m, v, sum(w.size for w in weights)))

    return jax.shard_map(
        step,
        mesh=mesh,
        in_specs=(P(("rep", "dp"), None, None),) * 2 + (P(None, None, None),) * 9,
        out_specs=(P("rep", None, None),) * 9,
        check_vma=False,
    )
```

```python
import functools
import jax
import jax.numpy as jnp
from jax import lax
from jax.experimental import pallas as pl
from jax.experimental.pallas import tpu as pltpu
from jax.sharding import PartitionSpec as P

MESH = pl.DeviceIdType.MESH
LANES = 128
BLOCK = 1024
PARTS = ((1.5, 0.7, 0.7, 0.4), (2.2, 1.2, 1.3, 0.7))
F32, BF16 = jnp.float32, jnp.bfloat16


def block_rows(n, most=256):
    return max(b for b in range(8, most + 1, 8) if n % b == 0)


def halves(c):
    a = (c // 2 + 15) // 16 * 16
    return a, c - a


class Plan:
    SLOTS = 3

    def __init__(self, units, run, tiles, side):
        self.side = side
        self.units = []
        self.rows = len({layer for layer, _ in units}) * tiles * run
        r1 = r2 = sem = 0
        most = max(count for _, count in units) * run // 2 // side
        row = {layer: layer * tiles * run for layer, _ in units}
        tile = {layer: 0 for layer, _ in units}
        for u, (layer, count) in enumerate(units):
            h = count * run // 2
            c1 = h // side
            c2 = c1 // side
            streams = []
            for s in range(2):
                acc = (2 * (u % self.SLOTS) + s) * most
                streams.append(dict(layer=layer, tile=tile[layer], count=count, base=row[layer] + s * h, h=h, c1=c1, c2=c2, r1=r1, r2=r2, sem=sem, acc=acc, s=s))
                r1 += 3 * c1
                r2 += 3 * c2
                sem += 20
            self.units.append(streams)
            row[layer] += 2 * h
            tile[layer] += count
        self.r1, self.r2, self.acc, self.sems = r1, r2, 2 * self.SLOTS * most, sem


class Comm:
    def __init__(self, plan, lg, gathered, r1, r2, acc, squares, send, recv):
        self.plan, self.lg, self.g, self.r1, self.r2, self.acc = plan, lg, gathered, r1, r2, acc
        self.squares, self.send, self.recv = squares, send, recv
        side = plan.side
        me = lax.axis_index("dp")
        self.x, self.y = me // side, me % side

    def at(self, ring, step):
        side = self.plan.side
        if ring == 0:
            return {"dp": lax.rem(self.x + (step + side), side) * side + self.y}
        return {"dp": self.x * side + lax.rem(self.y + (step + side), side)}

    def barrier(self):
        sem = pltpu.get_barrier_semaphore()
        for ring in range(2):
            for step in range(1, self.plan.side):
                pl.semaphore_signal(sem, inc=1, device_id=self.at(ring, step), device_id_type=MESH)
        pl.semaphore_wait(sem, 2 * (self.plan.side - 1))

    def copy(self, src, dst, k, device):
        return pltpu.make_async_remote_copy(
            src_ref=src, dst_ref=dst, send_sem=self.send.at[k], recv_sem=self.recv.at[k], device_id=device, device_id_type=MESH
        )

    def rs_message(self, st, phase, i):
        base, c, r, r0, k = self.geometry(st, phase)
        ring, _ = self.ring(st, phase)
        a, b = halves(c)
        step, off, n, slot, way = (
            (2, 0, a, r0, 1), (1, a, b, r0 + c + a, 1), (2, a, b, r0 + a, -1),
            (-1, 0, a, r0 + 2 * c, -1), (1, 0, a, r0 + c, 1), (-1, a, b, r0 + 2 * c + a, -1),
        )[i]
        return self.copy(self.rows(self.lg, self.place(st, phase, step) + off, n), self.rows(r, slot, n), k + i, self.at(ring, way))

    def ag_message(self, st, level, i):
        phase, base, c, k = self.ag_geometry(st, level)
        ring, _ = self.ring(st, phase)
        a, b = halves(c)
        step, off, n, way = ((0, 0, c, 1), (0, 0, c, -1), (-1, 0, a, 1), (1, a, b, -1))[i]
        part = self.rows(self.g, self.place(st, phase, step) + off, n)
        return self.copy(part, part, k + i, self.at(ring, way))

    def finish(self):
        for unit in self.plan.units:
            for st in unit:
                for which in range(2):
                    for i in range(6):
                        self.rs_message(st, which, i).wait_send()
                    for i in range(4):
                        self.ag_message(st, which, i).wait_send()

    def ring(self, st, phase):
        ring = st["s"] if phase == 0 else 1 - st["s"]
        return ring, (self.x if ring == 0 else self.y)

    def geometry(self, st, phase):
        side = self.plan.side
        if phase == 0:
            return st["base"], st["c1"], self.r1, st["r1"], st["sem"]
        _, p = self.ring(st, 0)
        return st["base"] + p * st["c1"], st["c2"], self.r2, st["r2"], st["sem"] + 6

    def rows(self, ref, start, n):
        return ref.at[pl.ds(pl.multiple_of(start, 8), n), :]

    def place(self, st, phase, step):
        base, c, *_ = self.geometry(st, phase)
        _, p = self.ring(st, phase)
        return base + lax.rem(p + (step + self.plan.side), self.plan.side) * c

    def rs_start(self, st, phase):
        for i in (0, 2, 1, 3):
            self.rs_message(st, phase, i).start()

    def add_loop(self, n, body):
        b = block_rows(n)

        def step(i, carry):
            body(i * b, b)
            return carry

        lax.fori_loop(0, n // b, step, 0)

    def load(self, ref, start, n):
        return ref[pl.ds(pl.multiple_of(start, 8), n), :]

    def rs_mid(self, st, phase):
        base, c, r, r0, k = self.geometry(st, phase)
        ring, p = self.ring(st, phase)
        a, b = halves(c)
        for which, step, off, n in ((0, 1, 0, a), (2, -1, a, b)):
            self.rs_message(st, phase, which).wait_recv()
            mine = self.place(st, phase, step) + off
            slot = r0 + off

            def body(o, m, mine=mine, slot=slot, off=off, step=step):
                if phase == 0:
                    own = self.load(self.lg, mine + o, m).astype(F32)
                else:
                    own = self.load(self.acc, st["acc"] + lax.rem(p + (step + self.plan.side), self.plan.side) * c + off + o, m)
                total = own + self.load(r, slot + o, m).astype(F32)
                self.lg[pl.ds(pl.multiple_of(mine + o, 8), m), :] = total.astype(BF16)

            self.add_loop(n, body)
            self.rs_message(st, phase, 4 if which == 0 else 5).start()

    def rs_end(self, st, phase):
        base, c, r, r0, k = self.geometry(st, phase)
        ring, p = self.ring(st, phase)
        for which in (1, 3, 4, 5):
            self.rs_message(st, phase, which).wait_recv()
        mine = base + p * c

        def body(o, m):
            if phase == 0:
                own = self.load(self.lg, mine + o, m).astype(F32)
            else:
                own = self.load(self.acc, st["acc"] + p * c + o, m)
            total = own + self.load(r, r0 + c + o, m).astype(F32) + self.load(r, r0 + 2 * c + o, m).astype(F32)
            if phase == 0:
                self.acc[pl.ds(pl.multiple_of(st["acc"] + o, 8), m), :] = total
                self.lg[pl.ds(pl.multiple_of(mine + o, 8), m), :] = total.astype(BF16)
            else:
                rounded = total.astype(BF16)
                self.g[pl.ds(pl.multiple_of(mine + o, 8), m), :] = rounded
                wide = rounded.astype(F32)
                self.squares[...] += jnp.sum((wide * wide).reshape(m // 8, 8, LANES), axis=0)

        self.add_loop(c, body)

    def ag_geometry(self, st, level):
        phase = 1 - level
        base, c, *_ = self.geometry(st, phase)
        return phase, base, c, st["sem"] + 12 + 4 * level

    def ag_start(self, st, level):
        for i in range(2):
            self.ag_message(st, level, i).start()

    def ag_mid(self, st, level):
        for i in range(2):
            self.ag_message(st, level, i).wait_recv()
            self.ag_message(st, level, 2 + i).start()

    def ag_end(self, st, level):
        for i in range(2, 4):
            self.ag_message(st, level, i).wait_recv()

    def norm_step(self, step, parts, send, recv):
        side = self.plan.side

        def messages(ring):
            here = parts.at[ring * side + (self.x if ring == 0 else self.y)]
            for far in range(1, side):
                k = ring * (side - 1) + far - 1
                yield pltpu.make_async_remote_copy(
                    src_ref=here, dst_ref=here, send_sem=send.at[k], recv_sem=recv.at[k], device_id=self.at(ring, far), device_id_type=MESH
                )

        if step > 0:
            for c in messages(step - 1):
                c.wait()
            total = parts[(step - 1) * side]
            for i in range(1, side):
                total = total + parts[(step - 1) * side + i]
            self.squares[...] = total
        if step < 2:
            parts[step * side + (self.x if step == 0 else self.y)] = self.squares[...]
            for c in messages(step):
                c.start()

    def step(self, st, step):
        if step == 0:
            self.rs_start(st, 0)
        elif step in (1, 3):
            self.rs_mid(st, step // 2)
        elif step == 2:
            self.rs_end(st, 0)
            self.rs_start(st, 1)
        elif step == 4:
            self.rs_end(st, 1)
            self.ag_start(st, 0)
        elif step in (5, 7):
            self.ag_mid(st, step // 7)
        elif step == 6:
            self.ag_end(st, 0)
            self.ag_start(st, 1)
        else:
            self.ag_end(st, 1)


def update(w, m, v, g, factor):
    g = g.astype(F32) * factor
    w = w.astype(F32)
    m = 0.9 * m + 0.1 * g
    v = 0.95 * v + 0.05 * g * g
    step = m * lax.rsqrt(v + 1e-8) + 0.1 * w
    return (w - 0.02 * step).astype(BF16), m, v


def dot(a, b):
    return jnp.dot(a, b, preferred_element_type=F32)


def dot_nt(a, b):
    return lax.dot_general(a, b, (((1,), (1,)), ((), ())), preferred_element_type=F32)


def row_loop(rows, block, body):
    def step(i, carry):
        body(pl.ds(pl.multiple_of(i * block, block), block))
        return carry

    lax.fori_loop(0, rows // block, step, 0)


def scale_of(wide):
    return lax.rsqrt(jnp.mean(wide * wide, -1, keepdims=True) + 1e-6)


def normalise(h, a, at):
    def body(rows):
        wide = h[rows, :].astype(F32)
        value = (wide * scale_of(wide)).astype(BF16)
        a[rows, :] = value
        at[:, rows] = value.T

    row_loop(h.shape[0], 256, body)


def transpose(src, dst):
    def body(rows):
        dst[:, rows] = src[rows, :].T

    row_loop(src.shape[0], 256, body)


def sigmoid(z):
    return 0.5 * jnp.tanh(0.5 * z) + 0.5


def column_tiles(ff):
    whole = ff // 256
    return [(i * 256, 256) for i in range(whole)] + ([(whole * 256, LANES)] if ff % 256 else [])


def forward(a, h, wg, wu, wd, out):
    def body(rows):
        block = a[rows, :]
        parts = []
        for start, width in column_tiles(wg.shape[1]):
            cols = pl.ds(start, width)
            gate, up = dot(block, wg[:, cols]), dot(block, wu[:, cols])
            parts.append((gate * sigmoid(gate) * up).astype(BF16))
        out[rows, :] = h[rows, :] + dot(jnp.concatenate(parts, axis=1), wd[...]).astype(BF16)

    row_loop(a.shape[0], 512, body)


def backward_tile(start, width, a, at, dy, dyt, wg, wu, wd, act, by_both, lg, row, by_input=None, pause=lambda part: None):
    cols = pl.ds(start, width)
    both = jnp.concatenate([wg[:, cols], wu[:, cols]], axis=1)
    down = wd[cols, :]

    def body(rows):
        hidden = dot(a[rows, :], both)
        gate, up = hidden[:, :width], hidden[:, width:]
        by_act = dot_nt(dy[rows, :], down).astype(BF16).astype(F32)
        s = sigmoid(gate)
        silu = gate * s
        act[rows, :width] = (silu * up).astype(BF16)
        by_gate = (by_act * up * (s + silu * (1.0 - s))).astype(BF16)
        by_up = (by_act * silu).astype(BF16)
        by_both[rows, :width] = by_gate
        by_both[rows, width : 2 * width] = by_up

    row_loop(a.shape[0], BLOCK, body)
    pause(0)
    if by_input is not None:

        def add(rows):
            by_input[rows, :] += dot_nt(by_both[rows, : 2 * width], both)

        row_loop(a.shape[0], BLOCK, add)
        pause(1)
    d = wg.shape[0]

    def inner(i, carry):
        out = dot(at[...], by_both[:, pl.ds(pl.multiple_of(i * width, LANES), width)]).astype(BF16)
        for j in range(width // LANES):
            lg[pl.ds(pl.multiple_of(row + j * 3 * d + i * d, 16), d), :] = out[:, j * LANES : (j + 1) * LANES]
        return carry

    lax.fori_loop(0, 2, inner, 0)
    pause(2)
    out = dot(dyt[...], act[:, :width]).astype(BF16).T
    for j in range(width // LANES):
        for c in range(d // LANES):
            lg[pl.ds(pl.multiple_of(row + j * 3 * d + 2 * d + c * LANES, 16), LANES), :] = out[j * LANES : (j + 1) * LANES, c * LANES : (c + 1) * LANES]
    pause(3)


def backward_input(h, dy, by_a, dyt):
    d = h.shape[1]

    def body(rows):
        by = by_a[rows, :].astype(BF16).astype(F32)
        wide = h[rows, :].astype(F32)
        s = scale_of(wide)
        by_scale = jnp.sum(by * wide, -1, keepdims=True)
        by_wide = by * s - wide * (by_scale * s * s * s * (1.0 / d))
        value = dy[rows, :] + by_wide.astype(BF16)
        dy[rows, :] = value
        dyt[:, rows] = value.T

    row_loop(h.shape[0], 256, body)


class Schedule:
    RATE, LATENCY, COST, BACKLOG = 44000.0, 2.8, 0.3, 12.0

    def __init__(self, units):
        self.units = units
        self.now = self.free = 0.0
        self.due = {}
        self.squares = None
        self.out = []

    def send(self, rows):
        self.free = max(self.now, self.free) + rows * LANES * 2 / self.RATE
        return self.free + self.LATENCY

    def begin(self, u):
        self.run(u, 0)

    def run(self, u, step):
        st = self.units[u][0]
        c1, c2 = st["c1"], st["c2"]
        self.out.append((u, step))
        self.now += self.COST * (1 if step in (1, 2) else 0.3)
        sent = {0: (c1 // 2, c1 // 2), 1: (c1 // 2,), 2: (c2 // 2, c2 // 2), 3: (c2 // 2,), 4: (c2,), 5: (c2 // 2,), 6: (c1,), 7: (c1 // 2,)}
        times = [self.send(rows) for rows in sent.get(step, ())]
        if step < 8:
            self.due[u] = (step + 1, times[0])
        else:
            del self.due[u]

    def norm(self, step):
        self.out.append(("norm", step))
        self.now += 0.1
        if step < 2:
            self.squares = (step + 1, self.send(64) + 1.5)
        else:
            self.squares = ("done", 0.0)

    def choices(self):
        found = [
            (due, 0 if step <= 4 else 1 if step != 6 else 2, u, step)
            for u, (step, due) in self.due.items()
            if step != 2 or self.due.get(u - Plan.SLOTS, (5, 0))[0] > 4
        ]
        if self.squares and self.squares[0] != "done":
            found.append((self.squares[1], 0, "norm", self.squares[0]))
        return found

    def take(self, which, step):
        if which == "norm":
            self.norm(step)
        else:
            self.run(which, step)

    def compute(self, us):
        self.now += us
        while True:
            ready = [c for c in self.choices() if c[0] <= self.now and (c[3] != 6 or self.free - self.now < self.BACKLOG)]
            if not ready:
                return
            _, _, which, step = min(ready, key=lambda c: (c[1], c[0]))
            self.take(which, step)

    def drain(self):
        begun = False
        while self.due or not begun or self.squares[0] != "done":
            if not begun and all(step > 4 for step, _ in self.due.values()):
                begun = True
                self.norm(0)
                continue
            late = [c for c in self.choices() if c[3] != 6 or self.free - self.now < self.BACKLOG or len(self.due) == 1] or self.choices()
            due, _, which, step = min(late, key=lambda c: (max(c[0], self.now), c[1], c[0]))
            self.now = max(self.now, due)
            self.take(which, step)


def step_kernel(plan, counts, x_h, dy_h, wg_h, wu_h, wd_h, gg_o, gu_o, gd_o, factor_out,
                h, dy, dyt, a, at, keep, wg, wu, wd, act, by_both, by_a,
                lg, gathered, r1, r2, acc, squares, parts, send, recv, nsend, nrecv, sem):
    comm = Comm(plan, lg, gathered, r1, r2, acc, squares, send, recv)
    layers, d, ff = wg.shape
    base = 3 * d * (ff // LANES)
    loads = [(x_h, h)] + [(w_h.at[0], w.at[0]) for w_h, w in ((wg_h, wg), (wu_h, wu), (wd_h, wd))]
    loads += [(w_h.at[1], w.at[1]) for w_h, w in ((wg_h, wg), (wu_h, wu), (wd_h, wd))]
    loads = [pltpu.make_async_copy(src, dst, sem.at[i]) for i, (src, dst) in enumerate(loads)]
    for c in loads:
        c.start()
    squares[...] = jnp.zeros_like(squares)
    comm.barrier()
    plan_at = Schedule(plan.units)
    plan_at.now = 21.0
    done = [0]

    def place(st, done):
        for t in range(st["tile"], st["tile"] + st["count"]):
            row, hidden = st["layer"] * base + t * 3 * d, pl.ds(t * LANES, LANES)
            pltpu.make_async_copy(gathered.at[pl.ds(row, d), :], gg_o.at[st["layer"], :, hidden], done).start()
            pltpu.make_async_copy(gathered.at[pl.ds(row + d, d), :], gu_o.at[st["layer"], :, hidden], done).start()
            for c in range(d // LANES):
                part = gathered.at[pl.ds(row + 2 * d + c * LANES, LANES), :]
                pltpu.make_async_copy(part, gd_o.at[st["layer"], hidden, pl.ds(c * LANES, LANES)], done).start()

    def steps(events):
        for which, step in events:
            if which == "norm":
                comm.norm_step(step, parts, nsend, nrecv)
                continue
            unit = plan.units[which]
            for st in unit:
                comm.step(st, step)
            if step == 8:
                place(unit[0], sem.at[len(loads) + 2 + which])

    def due():
        plan_at.compute(0.0)
        events = plan_at.out[done[0] :]
        done[0] = len(plan_at.out)
        return events

    def tiles(layer, by_input):
        first = sum(len(c) for c in counts[layer + 1 :])
        ends = {sum(counts[layer][: u + 1]): first + u for u in range(len(counts[layer]))}
        all_tiles = column_tiles(ff)
        events = []
        for start, width in all_tiles:
            mine = []
            for part, us in enumerate(PARTS[width > LANES]):
                plan_at.now += us if by_input or part != 1 else 0.0
                if part == 3 and (start + width) // LANES in ends:
                    plan_at.begin(ends[(start + width) // LANES])
                mine.append(due() if by_input or part != 1 else [])
            events.append(mine)

        def tile(start, width, number, pause):
            backward_tile(
                start, width, a, at, dy, dyt, wg.at[layer], wu.at[layer], wd.at[layer], act, by_both, lg,
                layer * base + number * 2 * 3 * d, by_a if by_input else None, pause,
            )

        whole = ff // 256

        def one(i, carry):
            def pause(part):
                for t in range(whole):
                    if events[t][part]:
                        pl.when(i == t)(functools.partial(steps, events[t][part]))

            tile(pl.multiple_of(i * 256, 256), 256, i, pause)
            return carry

        if by_input:
            by_a[...] = jnp.zeros_like(by_a)
        lax.fori_loop(0, whole, one, 0)
        for number in range(whole, len(all_tiles)):
            tile(*all_tiles[number], number, lambda part: steps(events[number][part]))

    loads[0].wait()
    normalise(h, a, at)
    for c in loads[1:4]:
        c.wait()
    forward(a, h, wg.at[0], wu.at[0], wd.at[0], keep)
    again = pltpu.make_async_copy(dy_h, dy, sem.at[len(loads)])
    again.start()
    normalise(keep, a, at)
    again.wait()
    transpose(dy, dyt)
    for c in loads[4:]:
        c.wait()
    tiles(1, True)
    again = pltpu.make_async_copy(x_h, h, sem.at[len(loads) + 1])
    again.start()
    backward_input(keep, dy, by_a, dyt)
    plan_at.now += 2.4
    steps(due())
    again.wait()
    normalise(h, a, at)
    plan_at.now += 2.4
    steps(due())
    tiles(0, False)
    plan_at.drain()
    steps(plan_at.out[done[0] :])
    total = jnp.sum(squares[...], axis=(0, 1), keepdims=True)
    factor = jnp.minimum(1.0, 0.5 * lax.rsqrt(total / (layers * 3 * d * ff) + 1e-30))
    factor_out[...] = jnp.broadcast_to(factor, factor_out.shape)
    for which, unit in enumerate(plan.units):
        rows = pl.ds(unit[0]["base"], 2 * unit[0]["h"])
        pltpu.make_async_copy(gathered.at[rows, :], lg.at[rows, :], sem.at[len(loads) + 2 + which]).wait()
    comm.finish()


def gradients(x, dy, wg, wu, wd, side):
    tokens, d = x.shape
    layers, _, ff = wg.shape
    tiles = ff // LANES
    counts = {layers - 1: [2, 4, 4, tiles - 10], 0: [4, 4, 4, tiles - 12]}
    plan = Plan([(layer, c) for layer in (layers - 1, 0) for c in counts[layer]], 3 * d, tiles, side)
    any_spec = pl.BlockSpec(memory_space=pl.ANY)
    flat, tall = pltpu.VMEM((tokens, d), BF16), pltpu.VMEM((d, tokens), BF16)
    tile = pltpu.VMEM((tokens, 256), BF16)
    return pl.pallas_call(
        functools.partial(step_kernel, plan, [counts[0], counts[layers - 1]]),
        name="gradients",
        out_shape=(*(jax.ShapeDtypeStruct(w.shape, BF16) for w in (wg, wu, wd)), jax.ShapeDtypeStruct((8, LANES), F32)),
        in_specs=[any_spec] * 5,
        out_specs=(*[any_spec] * 3, pl.BlockSpec(memory_space=pltpu.VMEM)),
        scratch_shapes=[
            flat, flat, tall, flat, tall, flat,
            pltpu.VMEM(wg.shape, BF16),
            pltpu.VMEM(wu.shape, BF16),
            pltpu.VMEM(wd.shape, BF16),
            tile,
            pltpu.VMEM((tokens, 512), BF16),
            pltpu.VMEM((tokens, d), F32),
            pltpu.VMEM((plan.rows, LANES), BF16),
            pltpu.VMEM((plan.rows, LANES), BF16),
            pltpu.VMEM((plan.r1, LANES), BF16),
            pltpu.VMEM((plan.r2, LANES), BF16),
            pltpu.VMEM((plan.acc, LANES), F32),
            pltpu.VMEM((8, LANES), F32),
            pltpu.VMEM((2 * side, 8, LANES), F32),
            pltpu.SemaphoreType.DMA((plan.sems,)),
            pltpu.SemaphoreType.DMA((plan.sems,)),
            pltpu.SemaphoreType.DMA((2 * (side - 1),)),
            pltpu.SemaphoreType.DMA((2 * (side - 1),)),
            pltpu.SemaphoreType.DMA((9 + len(plan.units),)),
        ],
        compiler_params=pltpu.CompilerParams(collective_id=0, has_side_effects=True, vmem_limit_bytes=67043328),
    )(x, dy, wg, wu, wd)


def solution(mesh):
    n = mesh.shape["dp"]
    side = int(n**0.5)

    def step(x, dy, *arrays):
        weights, m, v = (arrays[i : i + 3] for i in (0, 3, 6))
        *sums, factor = gradients(x[0], dy[0], *weights, side)
        new = [update(*one, factor[0, 0]) for one in zip(weights, m, v, sums, strict=True)]
        return tuple(one[which] for which in range(3) for one in new)

    return jax.shard_map(
        step,
        mesh=mesh,
        in_specs=(P(("rep", "dp"), None, None),) * 2 + (P(None, None, None),) * 9,
        out_specs=(P("rep", None, None),) * 9,
        check_vma=False,
    )
```
